32 devices in a mesh: band: 8 (over z, x), lev: 4 (over y, core).
Axes of the slice: x: 2, y: 2, z: 4, core: 2. Of those that a mesh axis runs over, the one named last changes fastest.
Arguments:
- checkpoints: float32 [4, 4, 32, 2, 256, 256], P(None, None, 'lev', None, 'band'), may hold values from -0.4 to 0.4
- final_cot: float32 [4, 32, 2, 256, 256], P(None, 'lev', None, 'band'), may hold values from -6 to 6
- obs_cot: float32 [4, 4, 32, 256, 512], P(None, None, None, 'band', 'lev'), may hold values from -0.2 to 0.2
- obs_time: int32 [4], replicated, may hold values from 0 to 3
- wave_order: int32 [256], replicated, may hold values from 0 to 255, each once
- legendre: bfloat16 [256, 256, 256], P('band'), may hold values from -0.375 to 0.375
- w_in: bfloat16 [128, 512], replicated, may hold values from -0.5 to 0.5
- w_out: bfloat16 [512, 128], replicated, may hold values from -0.25 to 0.25
- bias: float32 [512], replicated, may hold values from -3 to 3
Outputs:
- grad_state: float32 [4, 32, 2, 256, 256], P(None, 'lev', None, 'band')
- grad_w_in: float32 [128, 512], replicated
- grad_w_out: float32 [512, 128], replicated
- grad_bias: float32 [512], replicated
The draws below stay inside these ranges and needn't reach their ends.
Inputs may be any that keep to these rules, and one draw needn't show every extreme that they name: `obs_time`: each number names a step of the rollout. `wave_order`: each of the 256 zonal wavenumbers once.
All inputs are finite; a program needn't handle non-finite values.
Results may differ from the reference program's by a relative error of at most 0.014.
Values may be sent and summed in bfloat16 or wider, within the bound.
A program may use at most 192 MiB of HBM per device.

```python
import jax
import jax.numpy as jnp
from jax import lax

M = 256
LAT = 256
LON = 512
LEV = 32
VARS = 4
HID = 512
STEPS = 4
NOBS = 4


def plant(result, stream_key, least, largest):
    longest = result.shape.index(max(result.shape))
    spots = []
    for shift in (0, 1):
        where = [jax.random.randint(jax.random.fold_in(stream_key, axis), (), 0, length) for axis, length in enumerate(result.shape)]
        where[longest] = (where[longest] + shift) % result.shape[longest]
        spots.append(tuple(where))
    return result.at[spots[0]].set(least).at[spots[1]].set(largest)


def steps_of(rng, shape, shards, smallest, top_value):
    level = 1.0
    for position, parts in shards:
        steps = jax.random.uniform(jax.random.fold_in(jax.random.fold_in(rng, 6), position), (parts,), jnp.float32, smallest / len(shards), top_value / len(shards))
        level = level * jnp.repeat(jnp.exp(steps), shape[position] // parts).reshape((-1,) + (1,) * (len(shape) - 1 - position))
    return level


def bell_draw(stream_key, shape, width, limit, shards=(), kind=jnp.bfloat16):
    array = width * jax.random.normal(stream_key, shape, jnp.float32)
    if shards:
        array = array * steps_of(stream_key, shape, shards, -0.22, 0.18)
    return jnp.clip(array, -limit, limit).astype(kind)


def setup_inputs(seed: int = 0) -> dict:
    arg_keys = jax.random.split(jax.random.key(seed), 10)
    checkpoints = bell_draw(arg_keys[0], (STEPS, VARS, LEV, 2, M, M), 0.05, 0.4, ((2, 4), (4, 8)), jnp.float32)
    final_cot = bell_draw(arg_keys[1], (VARS, LEV, 2, M, M), 1.0, 6.0, ((1, 4), (3, 8)), jnp.float32)
    obs_cot = bell_draw(arg_keys[2], (NOBS, VARS, LEV, LAT, LON), 0.03, 0.2, ((3, 8), (4, 4)), jnp.float32)
    obs_time = plant(jax.random.randint(arg_keys[3], (NOBS,), 0, STEPS), jax.random.fold_in(arg_keys[3], 1), 0, STEPS - 1).astype(jnp.int32)
    wave_order = jax.random.permutation(arg_keys[4], M).astype(jnp.int32)
    legendre = bell_draw(arg_keys[5], (M, LAT, M), M ** -0.5, 0.375, ((0, 8),))
    w_in = bell_draw(arg_keys[6], (VARS * LEV, HID), (VARS * LEV) ** -0.5, 0.5)
    w_out = bell_draw(arg_keys[7], (HID, VARS * LEV), HID ** -0.5, 0.25)
    bias = bell_draw(arg_keys[8], (HID,), 0.5, 3.0, (), jnp.float32)
    return dict(checkpoints=checkpoints, final_cot=final_cot, obs_cot=obs_cot, obs_time=obs_time, wave_order=wave_order, legendre=legendre, w_in=w_in, w_out=w_out, bias=bias)


highest = lax.Precision.HIGHEST
dt_scale = 1.0


def lowered(values):
    return lax.optimization_barrier(values.astype(jnp.bfloat16)).astype(jnp.float32)


def tables(wave_order, lon_count):
    longitude = jnp.arange(lon_count, dtype=jnp.int32)
    phase_index = (wave_order[:, None] * longitude[None, :]) % lon_count
    angles = (2.0 * jnp.pi / lon_count) * phase_index.astype(jnp.float32)
    return lowered(jnp.cos(angles)), lowered(jnp.sin(angles))


def synth_legendre(masked, spectral):
    return lowered(jnp.einsum('rjn,vlcrn->vlcrj', masked, lowered(spectral), precision=highest))


def synth_fourier(coefficients, factor, cosine_table, sine_table):
    real_part = coefficients[:, :, 0] * factor[None, None, :, None]
    imag_part = coefficients[:, :, 1] * factor[None, None, :, None]
    return (jnp.einsum('vlrj,ro->vljo', real_part, cosine_table, precision=highest)
            - jnp.einsum('vlrj,ro->vljo', imag_part, sine_table, precision=highest))


def adjoint_fourier(grid_field, factor, cosine_table, sine_table):
    real_part = jnp.einsum('vljo,ro->vlrj', grid_field, cosine_table, precision=highest) * factor[:, None]
    imag_part = -jnp.einsum('vljo,ro->vlrj', grid_field, sine_table, precision=highest) * factor[:, None]
    return lowered(jnp.stack([real_part, imag_part], axis=2))


def adjoint_legendre(masked, coefficients):
    return jnp.einsum('rjn,vlcrj->vlcrn', masked, coefficients, precision=highest)


def reference(checkpoints, final_cot, obs_cot, obs_time, wave_order, legendre, w_in, w_out, bias):
    degrees = jnp.arange(M, dtype=jnp.int32)
    upper_mask = (degrees[None, None, :] >= wave_order[:, None, None]).astype(jnp.float32)
    masked = legendre.astype(jnp.float32) * upper_mask
    cosine_table, sine_table = tables(wave_order, LON)
    weight_m = jnp.where(wave_order == 0, 1.0, 2.0).astype(jnp.float32)
    inverse_lon = jnp.full((M,), 1.0 / LON, jnp.float32)
    degree_float = degrees.astype(jnp.float32)
    damping = 1.0 / (1.0 + 2.0 * degree_float * (degree_float + 1.0) / (M * M))
    feature_count = VARS * LEV
    column_count = LAT * LON
    adjoint = final_cot
    grad_w_in = jnp.zeros((feature_count, HID), jnp.float32)
    grad_w_out = jnp.zeros((HID, feature_count), jnp.float32)
    grad_bias = jnp.zeros((HID,), jnp.float32)
    for step in reversed(range(STEPS)):
        damped = damping * adjoint
        state_grid = synth_fourier(synth_legendre(masked, checkpoints[step]), weight_m, cosine_table, sine_table)
        features = state_grid.astype(jnp.bfloat16).reshape(feature_count, column_count)
        tangent_grid = synth_fourier(synth_legendre(masked, dt_scale * damped), inverse_lon, cosine_table, sine_table)
        tangent = tangent_grid.astype(jnp.bfloat16).reshape(feature_count, column_count)
        preact = jnp.dot(w_in.T, features, preferred_element_type=jnp.float32) + bias[:, None]
        logistic = jax.nn.sigmoid(preact)
        hidden = (preact * logistic).astype(jnp.bfloat16)
        hidden_grad = jnp.dot(w_out, tangent, preferred_element_type=jnp.float32)
        preact_grad = hidden_grad * (logistic * (1.0 + preact * (1.0 - logistic)))
        preact_low = preact_grad.astype(jnp.bfloat16)
        grad_w_out = grad_w_out + jnp.dot(hidden, tangent.T, preferred_element_type=jnp.float32)
        grad_w_in = grad_w_in + jnp.dot(features, preact_low.T, preferred_element_type=jnp.float32)
        grad_bias = grad_bias + jnp.sum(preact_grad, axis=1)
        column_grad = jnp.dot(w_in, preact_low, preferred_element_type=jnp.float32).reshape(VARS, LEV, LAT, LON)
        obs_weight = (obs_time == step).astype(jnp.float32)
        column_grad = column_grad + jnp.einsum('i,ivljo->vljo', obs_weight, obs_cot, precision=highest)
        back = adjoint_fourier(lowered(column_grad), weight_m, cosine_table, sine_table)
        adjoint = damped + adjoint_legendre(masked, back)
    return adjoint, grad_w_in, grad_w_out, grad_bias
```

```python
import jax
import jax.numpy as jnp
from jax import lax
from jax.sharding import PartitionSpec as P

dt_scale = 1.0


def tables(wave_order, lon_count):
    longitude = jnp.arange(lon_count, dtype=jnp.int32)
    phase_index = wave_order[:, None] * longitude[None, :] % lon_count
    angles = 2.0 * jnp.pi / lon_count * phase_index.astype(jnp.float32)
    return (jnp.cos(angles).astype(jnp.bfloat16), jnp.sin(angles).astype(jnp.bfloat16))


def rows_to_bands(sums, band_count):
    waves, lat, parts, steps, fields = sums.shape
    sums = sums.reshape(waves, band_count, lat // band_count, parts, steps, fields)
    return sums.transpose(1, 0, 3, 4, 2, 5).reshape(band_count, waves * parts, -1)


def synth_legendre(masked, spectral):
    return jnp.einsum(
        "rjn,svcrn->rjcsv",
        masked,
        spectral.astype(jnp.bfloat16),
        preferred_element_type=jnp.float32,
    ).astype(jnp.bfloat16)


def to_columns(masked, spectral, table, band_count, level_count, local_lat):
    steps, fields, local_levels = spectral.shape[:3]
    flat = spectral.reshape((steps, fields * local_levels) + spectral.shape[3:])
    sums = rows_to_bands(synth_legendre(masked, flat), band_count)
    rows = lax.all_to_all(sums, "band", split_axis=0, concat_axis=0, tiled=True)
    rows = rows.reshape(table.shape[0], -1)
    grid = jnp.einsum("kx,ko->xo", rows, table, preferred_element_type=jnp.float32).astype(
        jnp.bfloat16
    )
    grid = grid.reshape(steps, local_lat, fields * local_levels, level_count, -1)
    grid = grid.transpose(3, 0, 1, 2, 4)
    cols = lax.all_to_all(grid, "lev", split_axis=0, concat_axis=0, tiled=True)
    cols = cols.reshape(level_count, steps, local_lat, fields, local_levels, -1)
    cols = cols.transpose(1, 2, 3, 0, 4, 5)
    return cols.reshape(steps, local_lat, fields * level_count * local_levels, -1)


def network_grads(features, tangent, w_in, w_out, bias):
    preact = jnp.einsum("fh,jfo->jho", w_in, features, preferred_element_type=jnp.float32)
    preact = preact + bias[None, :, None]
    logistic = jax.nn.sigmoid(preact)
    hidden = (preact * logistic).astype(jnp.bfloat16)
    hidden_grad = jnp.einsum("hf,jfo->jho", w_out, tangent, preferred_element_type=jnp.float32)
    preact_grad = hidden_grad * (logistic * (1.0 + preact * (1.0 - logistic)))
    preact_low = preact_grad.astype(jnp.bfloat16)
    out_grad = jnp.einsum("jho,jfo->hf", hidden, tangent, preferred_element_type=jnp.float32)
    in_grad = jnp.einsum("jfo,jho->fh", features, preact_low, preferred_element_type=jnp.float32)
    bias_grad = jnp.sum(preact_grad, axis=(0, 2))
    column_grad = jnp.einsum("fh,jho->fjo", w_in, preact_low, preferred_element_type=jnp.float32)
    return (in_grad, out_grad, bias_grad, column_grad)


def reduce_grads(in_grad, out_grad, bias_grad):
    axes = ("band", "lev")
    devices = lax.axis_size(axes)
    feature_count, hidden_count = in_grad.shape
    rows = 2 * feature_count + 1
    padding = -rows % devices
    packed = jnp.concatenate(
        [
            in_grad,
            out_grad.T,
            bias_grad[None],
            jnp.zeros((padding, hidden_count), jnp.float32),
        ]
    )
    packed = packed.reshape(devices, -1, hidden_count)
    parts = lax.all_to_all(packed, axes, split_axis=0, concat_axis=0, tiled=True)
    total = lax.all_gather(jnp.sum(parts, axis=0), axes, axis=0, tiled=True)
    return (
        total[:feature_count],
        total[feature_count : 2 * feature_count].T,
        total[2 * feature_count],
    )


def shards(checkpoints, final_cot, obs_cot, obs_time, wave_order, legendre, w_in, w_out, bias):
    level_count = lax.axis_size("lev")
    band_count = lax.axis_size("band")
    local_waves, lat_count, wave_count = legendre.shape
    field_count, local_levels = final_cot.shape[:2]
    local_lat, local_lon = obs_cot.shape[3:]
    lon_count = local_lon * level_count
    step_count = checkpoints.shape[0]
    row_start = lax.axis_index("band") * local_waves
    my_waves = lax.dynamic_slice_in_dim(wave_order, row_start, local_waves)
    degrees = jnp.arange(wave_count, dtype=jnp.int32)
    upper_mask = degrees[None, None, :] >= my_waves[:, None, None]
    masked = jnp.where(upper_mask, legendre, jnp.zeros_like(legendre))
    cosine_table, sine_table = tables(wave_order, lon_count)
    table = jnp.stack([cosine_table, -sine_table], axis=1).reshape(2 * wave_count, lon_count)
    weight_m = jnp.where(wave_order == 0, 1.0, 2.0).astype(jnp.bfloat16)
    state_table = table * jnp.repeat(weight_m, 2)[:, None]
    tangent_table = table * jnp.asarray(1.0 / lon_count, jnp.bfloat16)
    degree_float = degrees.astype(jnp.float32)
    damping = 1.0 / (1.0 + 2.0 * degree_float * (degree_float + 1.0) / (wave_count * wave_count))
    state_columns = to_columns(
        masked, checkpoints, state_table, band_count, level_count, local_lat
    )
    adjoint = final_cot
    grads = None
    for step in reversed(range(step_count)):
        damped = damping * adjoint
        tangent = to_columns(
            masked, dt_scale * damped[None], tangent_table, band_count, level_count, local_lat
        )[0]
        in_grad, out_grad, bias_grad, column_grad = network_grads(
            state_columns[step], tangent, w_in, w_out, bias
        )
        new = (in_grad, out_grad, bias_grad)
        grads = new if grads is None else tuple(x + y for x, y in zip(grads, new))
        obs_sum = sum(
            jnp.where(obs_time[i] == step, obs_cot[i], 0.0) for i in range(obs_cot.shape[0])
        )
        column_grad = column_grad.reshape(obs_sum.shape) + obs_sum
        column_grad = column_grad.astype(jnp.bfloat16).reshape(
            field_count, level_count, local_levels, local_lat, local_lon
        )
        send = column_grad.transpose(1, 0, 2, 3, 4)
        level_grad = lax.all_to_all(send, "lev", split_axis=0, concat_axis=0, tiled=True)
        level_grad = level_grad.transpose(1, 2, 3, 0, 4).reshape(-1, lon_count)
        back = jnp.einsum(
            "ko,xo->kx", state_table, level_grad, preferred_element_type=jnp.float32
        ).astype(jnp.bfloat16)
        back = back.reshape(band_count, 2 * local_waves, -1)
        back = lax.all_to_all(back, "band", split_axis=0, concat_axis=0, tiled=True)
        back = back.reshape(
            band_count, local_waves, 2, field_count, local_levels, local_lat
        )
        back = back.transpose(1, 2, 3, 4, 0, 5).reshape(
            local_waves, 2, field_count, local_levels, lat_count
        )
        adjoint = damped + jnp.einsum(
            "rjn,rcvlj->vlcrn", masked, back, preferred_element_type=jnp.float32
        )
    return (adjoint,) + reduce_grads(*grads)


def solution(mesh):
    placed = (
        P(None, None, "lev", None, "band", None),
        P(None, "lev", None, "band", None),
        P(None, None, None, "band", "lev"),
        P(),
        P(),
        P("band", None, None),
        P(),
        P(),
        P(),
    )
    return jax.shard_map(
        shards,
        mesh=mesh,
        in_specs=placed,
        out_specs=(P(None, "lev", None, "band", None), P(), P(), P()),
        check_vma=False,
    )
```
